32 devices in a mesh: rep: 4 (over z), fsdp: 8 (over y, x, core).
Axes of the slice: x: 2, y: 2, z: 4, core: 2. Of those that a mesh axis runs over, the one named last changes fastest.
Arguments:
- tokens: bfloat16 [16384, 2048], P(('rep', 'fsdp')), may hold values from -6 to 6
- norm_gain: float32 [2048], replicated, may hold values from 0.5 to 1.5
- outer_params: float32 [2, 2048, 4096], P(None, 'fsdp'), may hold values from -6 to 6
- momentum: float32 [2, 2048, 4096], P(None, 'fsdp'), may hold values from -6 to 6
- deltas: bfloat16 [4, 2, 2048, 4096], P('rep', None, 'fsdp'), may hold values from -6 to 6
Outputs:
- new_params: float32 [2, 2048, 4096], P(None, 'fsdp')
- new_momentum: float32 [2, 2048, 4096], P(None, 'fsdp')
- hidden: bfloat16 [16384, 4096], P(('rep', 'fsdp'))
The draws below stay inside these ranges and needn't reach their ends.
All inputs are finite; a program needn't handle non-finite values.
Results may differ from the reference program's by a relative error of at most 0.01.
Values may be sent and summed in bfloat16 or wider, within the bound.
A program may use at most 192 MiB of HBM per device.

```python
import math
import jax
import jax.numpy as jnp
from jax import lax

D = 2048
FF = 4096
TOKENS = 16384
N_REP = 4


def block_levels(stream_key, shape, split, least, largest):
    def one(position, blocks):
        heights = jax.random.uniform(jax.random.fold_in(jax.random.fold_in(stream_key, 6), position), (blocks,), jnp.float32, least / len(split), largest / len(split))
        return jnp.repeat(jnp.exp(heights), shape[position] // blocks).reshape((-1,) + (1,) * (len(shape) - position - 1))

    loudness = one(*split[0])
    for cut in split[1:]:
        loudness = loudness * one(*cut)
    return loudness


def normal_values(stream_key, dims, deviation, most, pieces=(), held_as=jnp.bfloat16):
    values = jax.random.normal(stream_key, dims, jnp.float32) * deviation
    if len(pieces) > 0:
        values = block_levels(stream_key, dims, pieces, -0.22, 0.18) * values
    return jnp.clip(values, min=-most, max=most).astype(held_as)


def setup_inputs(seed: int = 0) -> dict:
    key_list = jax.random.split(jax.random.key(seed), 6)
    return {
        "tokens": normal_values(key_list[0], (TOKENS, D), 1.0, 6.0, ((0, 32),)),
        "norm_gain": jnp.clip(1.0 + 0.1 * jax.random.normal(key_list[1], (D,), jnp.float32), 0.5, 1.5),
        "outer_params": normal_values(key_list[2], (2, D, FF), 1.0, 6.0, ((1, 8),), jnp.float32),
        "momentum": normal_values(key_list[3], (2, D, FF), 0.5, 6.0, ((1, 8),), jnp.float32),
        "deltas": normal_values(key_list[4], (N_REP, 2, D, FF), 0.5, 6.0, ((0, 4), (2, 8))),
    }


EPS = 1e-05
MU = 0.9
RATE = 0.7

def reference(tokens, norm_gain, outer_params, momentum, deltas):
    total = jnp.zeros(outer_params.shape, jnp.float32)
    for group in range(N_REP):
        total = total + deltas[group].astype(jnp.float32)
    outer_grad = total / N_REP
    new_momentum = MU * momentum + outer_grad
    new_params = outer_params - RATE * (outer_grad + MU * new_momentum)
    weights = new_params.astype(jnp.bfloat16)
    values = tokens.astype(jnp.float32)
    scale_rows = lax.rsqrt(lax.optimization_barrier(jnp.mean(values * values, axis=-1, keepdims=True)) + EPS)
    normed = (values * scale_rows * norm_gain).astype(jnp.bfloat16)
    factor = 1.0 / math.sqrt(D)
    gate = jnp.dot(normed, weights[0], preferred_element_type=jnp.float32) * factor
    up = jnp.dot(normed, weights[1], preferred_element_type=jnp.float32) * factor
    hidden = (jax.nn.silu(gate) * up).astype(jnp.bfloat16)
    return (new_params, new_momentum, hidden)
```

```python
import functools
import math

import jax
import jax.numpy as jnp
from jax import lax
from jax.experimental import pallas as pl
from jax.experimental.pallas import tpu as pltpu
from jax.sharding import PartitionSpec as P

EPS = 1e-05
MU = 0.9
RATE = 0.7
CORES = 2
LANES = 4
WIDTH = 128
PARTS = 4
EARLY = 3
LATE_AT = 4
PASS_AT = (4, 7, 10, 14)
SUM_LAG = 1
STEP_LAG = 2
PASS_LAG = 5
DOT_LAG = 4


def advance(params, moment, summed, groups):
    outer_grad = summed * (1.0 / groups)
    moment_next = MU * moment + outer_grad
    params_next = params - RATE * (outer_grad + MU * moment_next)
    return (params_next, moment_next)


def other(bit, turned):
    return 1 - bit if turned else bit


def kernel(
    groups, shards, z_rows,
    tokens, gain, params, moment, deltas,
    p_out, m_out, hid_out,
    toks, weights, stage, own, peer_in, total, h_x, h_z,
    load_sem, token_sem, p_sem, m_sem,
    part_recv, peer_recv, total_recv, part_send, total_send,
    tx_recv, tx_send, tz_recv, tz_send, pair_recv, diag_recv, pair_send,
    lane_recv, lane_send, far_recv, far_send, h_recv, h_send,
):
    pieces, _, height, width = own.shape
    chunks = pieces // LANES
    rows, model = tokens.shape
    x_rows = rows - z_rows
    z_base = LANES * x_rows
    quarter = chunks * width
    quads = shards // LANES
    bf16, f32 = jnp.bfloat16, jnp.float32
    rep = lax.axis_index("rep")
    mine = lax.axis_index("fsdp")
    core = mine % CORES
    chip = mine // CORES
    x_bit = chip % 2
    quad = chip // 2
    turn = ((rep + 1) // 2) % 2
    lane = ((x_bit + turn) % 2) * 2 + core
    middle = groups // 2
    low = rep < middle
    inward = jnp.where(low, rep + 1, rep - 1)
    outward = jnp.where(low, rep - 1, rep + 1)
    at_end = (rep == 0) | (rep == groups - 1)
    at_middle = (rep == middle - 1) | (rep == middle)
    z_pair = rep + 1 - 2 * (rep % 2)

    def shard(bit, which_core, where=quad):
        return (where * 2 + bit) * CORES + which_core

    def at_x(k):
        return shard(other(x_bit, k // 2), other(core, k % 2))

    def remote(src, dst, send, recv, **device):
        return pltpu.make_async_remote_copy(
            src_ref=src, dst_ref=dst, send_sem=send, recv_sem=recv,
            device_id=device, device_id_type=pl.DeviceIdType.MESH)

    def z_device(k):
        near = {"fsdp": chip * CORES + other(core, k % 2)}
        return {"rep": z_pair, **near} if k // 2 else near

    def high(i):
        return (LANES - 1 - i) // 2

    def odd(i):
        return (LANES - 1 - i) % 2

    def columns(c, i):
        h = other(x_bit, high(i)) * 2 + other(core, odd(i))
        return pl.ds(pl.multiple_of(h * quarter + c * width, width), width)

    def away(i):
        return (high(i) + turn) % 2

    def lane_shard(i, where=quad):
        return shard((x_bit + high(i) + turn) % 2, other(core, odd(i)), where)

    def block(c, owner):
        return weights.at[c, pl.ds(pl.multiple_of(owner * height, height), height), :]

    def delta_load(c, i):
        n = c * LANES + i
        return pltpu.make_async_copy(deltas.at[0, :, :, columns(c, i)], own.at[n], load_sem.at[n])

    def part_copy(dst, n, recv):
        return remote(own.at[n], dst.at[n], part_send, recv.at[n], rep=inward)

    def total_copy(n):
        return remote(total.at[n], total.at[n], total_send, total_recv.at[n], rep=outward)

    def lane_copy(c, i):
        return remote(stage.at[c * LANES + i], block(c, mine), lane_send, lane_recv.at[c, i], fsdp=lane_shard(i))

    def far_copy(c, i, r):
        at = block(c, lane_shard(i))
        return remote(at, at, far_send, far_recv.at[c], fsdp=shard(x_bit, core, (quad + r) % quads))

    part_rows = x_rows // PARTS

    def x_part(k, j):
        return toks.at[pl.ds(k * x_rows + j * part_rows, part_rows), :]

    def z_part(k):
        return toks.at[pl.ds(z_base + k * z_rows, z_rows), :]

    def token_x(j):
        return remote(x_part(0, j), x_part(2, j), tx_send, tx_recv.at[j], fsdp=at_x(2))

    def token_pass(j):
        return remote(x_part(2, j), x_part(3, j), pair_send, diag_recv.at[0], fsdp=at_x(1))

    def token_z():
        return remote(z_part(0), z_part(2), tz_send, tz_recv, rep=z_pair)

    def token_z_pass():
        return remote(z_part(2), z_part(3), pair_send, diag_recv.at[1], fsdp=at_x(1))

    token_copies = (
        pltpu.make_async_copy(tokens.at[pl.ds(0, x_rows), :], toks.at[pl.ds(0, x_rows), :], token_sem.at[0]),
        pltpu.make_async_copy(tokens.at[pl.ds(x_rows, z_rows), :], z_part(0), token_sem.at[1]),
    )
    for copy in token_copies:
        copy.start()

    @pl.loop(0, chunks)
    def _(c):
        for i in range(LANES):
            delta_load(c, i).start()

    p_load = pltpu.make_async_copy(params, p_out, p_sem)
    m_load = pltpu.make_async_copy(moment, m_out, m_sem)
    p_load.start()
    m_load.start()

    barrier = pltpu.get_barrier_semaphore()
    greeted = 0
    for k in (1, 2, 3):
        pl.semaphore_signal(barrier, inc=1, device_id={"fsdp": at_x(k)}, device_id_type=pl.DeviceIdType.MESH)
    for r in range(1, quads):
        pl.semaphore_signal(
            barrier, inc=1, device_id={"fsdp": shard(x_bit, core, (quad + r) % quads)}, device_id_type=pl.DeviceIdType.MESH)
    pl.semaphore_signal(barrier, inc=1, device_id=z_device(3), device_id_type=pl.DeviceIdType.MESH)
    pl.semaphore_signal(barrier, inc=1, device_id={"rep": inward}, device_id_type=pl.DeviceIdType.MESH)
    greeted = LANES - 1 + quads - 1 + 2

    @pl.when(jnp.logical_not(at_end))
    def _():
        pl.semaphore_signal(barrier, inc=1, device_id={"rep": outward}, device_id_type=pl.DeviceIdType.MESH)

    for copy in token_copies:
        copy.wait()
    piece = 32

    def normalize(first, count):
        @pl.loop(0, count // piece)
        def _(i):
            at = pl.ds(pl.multiple_of(first + i * piece, piece), piece)
            values = toks[at, :].astype(f32)
            scale = lax.rsqrt(jnp.mean(values * values, axis=-1, keepdims=True) + EPS)
            toks[at, :] = (values * scale * gain[...]).astype(bf16)

    normalize(0, x_rows)
    normalize(z_base, z_rows)

    @pl.when(jnp.logical_not(at_end))
    def _():
        pl.semaphore_wait(barrier, greeted + 1)

    @pl.when(at_end)
    def _():
        pl.semaphore_wait(barrier, greeted)

    for j in range(EARLY):
        token_x(j).start()

    @pl.when(jnp.logical_not(at_end))
    def _():
        token_z().start()

    @pl.loop(0, chunks)
    def _(c):
        for i in range(LANES):
            n = c * LANES + i
            pltpu.make_async_copy(own.at[n], own.at[n], load_sem.at[n]).wait()

            @pl.when(at_end & jnp.logical_not(at_middle))
            def _(n=n):
                part_copy(total, n, part_recv).start()

            @pl.when(at_end & at_middle)
            def _(n=n):
                part_copy(peer_in, n, peer_recv).start()

    @pl.when(at_end)
    def _():
        token_z().start()

    remote(toks.at[pl.ds(0, x_rows), :], toks.at[pl.ds(x_rows, x_rows), :], pair_send, pair_recv.at[0], fsdp=at_x(1)).start()
    remote(z_part(0), z_part(1), pair_send, pair_recv.at[1], fsdp=at_x(1)).start()

    factor = 1.0 / math.sqrt(model)

    def gated(at, c):
        both = jnp.dot(toks[at, :], weights[c], preferred_element_type=f32) * factor
        gate, up = both[:, :width], both[:, width:]
        return (gate / (1.0 + jnp.exp(-gate)) * up).astype(bf16)

    def live(c):
        return (c >= 0) & (c < chunks)

    def shifted(t, i, lag):
        return t + (i - lag) // LANES, (i - lag) % LANES

    def gather_in(c, i):
        n = c * LANES + i
        part_copy(total, n, part_recv).wait_recv()
        own[n] = (own[n].astype(f32) + total[n].astype(f32)).astype(bf16)

        @pl.when(at_middle)
        def _():
            part_copy(peer_in, n, peer_recv).start()

        @pl.when(jnp.logical_not(at_middle))
        def _():
            part_copy(total, n, part_recv).start()

    def join(c, i):
        n = c * LANES + i
        part_copy(peer_in, n, peer_recv).wait_recv()
        total[n] = (own[n].astype(f32) + peer_in[n].astype(f32)).astype(bf16)

        @pl.when(jnp.logical_not(at_end))
        def _():
            total_copy(n).start()

    def update(c, i):
        n = c * LANES + i

        @pl.when(jnp.logical_not(at_middle))
        def _():
            total_copy(n).wait_recv()

            @pl.when(jnp.logical_not(at_end))
            def _():
                total_copy(n).start()

        if i == 0:
            @pl.when(c == 0)
            def _():
                p_load.wait()
                m_load.wait()

        at = columns(c, i)
        for which in range(2):
            stepped, moved = advance(p_out[which, :, at], m_out[which, :, at], total[n, which].astype(f32), groups)
            p_out[which, :, at] = stepped
            m_out[which, :, at] = moved
            stage[n, :, which * width:(which + 1) * width] = stepped.astype(bf16)
        if odd(i):
            lane_copy(c, i).start()
        else:
            @pl.when(away(i) == 1)
            def _():
                lane_copy(c, i).start()

            @pl.when(away(i) == 0)
            def _():
                start = pl.multiple_of(mine * height, height)
                weights[c, pl.ds(start, height), :] = stage[n]

    def pass_on(c, i):
        if odd(i):
            lane_copy(c, i).wait_recv()
        else:
            @pl.when(away(i) == 1)
            def _():
                lane_copy(c, i).wait_recv()
        for r in range(1, quads):
            far_copy(c, i, r).start()

    def project(c, k):
        hidden = gated(slice(k * x_rows, (k + 1) * x_rows), c)
        slot = lane * chunks + c
        if k == 0:
            hid_out[slot, 0:x_rows, :] = hidden
        else:
            h_x[c, k - 1] = hidden
            remote(h_x.at[c, k - 1], hid_out.at[slot, pl.ds(0, x_rows), :], h_send.at[0], h_recv.at[0], fsdp=at_x(k)).start()

    def project_z(c):
        hidden = gated(slice(z_base, z_base + LANES * z_rows), c)
        slot = lane * chunks + c
        hid_out[slot, x_rows:rows, :] = hidden[0:z_rows]
        h_z[c] = hidden[z_rows:]
        for k in (3, 2, 1):
            remote(h_z.at[c, pl.ds((k - 1) * z_rows, z_rows), :], hid_out.at[slot, pl.ds(x_rows, z_rows), :],
                   h_send.at[1], h_recv.at[1], **z_device(k)).start()

    tail_z = -(-chunks // DOT_LAG)

    @pl.loop(0, chunks + DOT_LAG)
    def _(t):
        for i in range(LANES):
            @pl.when((t < chunks) & jnp.logical_not(at_end))
            def _(i=i):
                gather_in(t, i)

            for stepper, lag, when in ((join, SUM_LAG, at_middle), (update, STEP_LAG, None), (pass_on, PASS_LAG, None)):
                c, at = shifted(t, i, lag)

                @pl.when(live(c) if when is None else live(c) & when)
                def _(stepper=stepper, c=c, at=at):
                    stepper(c, at)

            if LATE_AT % LANES == i:
                @pl.when(t == LATE_AT // LANES)
                def _():
                    for j in range(EARLY, PARTS):
                        token_x(j).start()

            for j in range(PARTS):
                if PASS_AT[j] % LANES == i:
                    @pl.when(t == PASS_AT[j] // LANES)
                    def _(j=j):
                        token_x(j).wait_recv()
                        token_pass(j).start()

            @pl.when(live(t - DOT_LAG))
            def _(i=i):
                c = t - DOT_LAG
                if i == 0:
                    @pl.when(c == 0)
                    def _():
                        there = toks.at[pl.ds(x_rows, x_rows), :]
                        pltpu.make_async_copy(there, there, pair_recv.at[0]).wait()
                        pltpu.make_async_copy(there, there, diag_recv.at[0]).wait()

                    for _ in range(1, quads):
                        arrived = weights.at[c, pl.ds(0, LANES * height), :]
                        pltpu.make_async_copy(arrived, arrived, far_recv.at[c]).wait()
                project(c, LANES - 1 - i)

        @pl.when(t == chunks)
        def _():
            token_z().wait_recv()
            token_z_pass().start()
            pltpu.make_async_copy(z_part(1), z_part(1), pair_recv.at[1]).wait()
            pltpu.make_async_copy(z_part(3), z_part(3), diag_recv.at[1]).wait()

        @pl.when(t >= chunks)
        def _():
            first = (t - chunks) * tail_z

            @pl.loop(first, jnp.minimum(first + tail_z, chunks))
            def _(c):
                project_z(c)

    got = hid_out.at[pl.ds(0, (LANES - 1) * chunks), pl.ds(0, x_rows), :]
    pltpu.make_async_copy(got, got, h_recv.at[0]).wait()
    got = hid_out.at[pl.ds(0, (LANES - 1) * chunks), pl.ds(x_rows, z_rows), :]
    pltpu.make_async_copy(got, got, h_recv.at[1]).wait()
    pltpu.make_async_copy(h_x, h_x, h_send.at[0]).wait()
    pltpu.make_async_copy(h_z, h_z, h_send.at[1]).wait()
    pltpu.make_async_copy(own, own, part_send).wait()

    @pl.when(jnp.logical_not(at_end))
    def _():
        pltpu.make_async_copy(total, total, total_send).wait()

    sent = stage.at[pl.ds(0, (LANES - 1) * chunks)]
    pltpu.make_async_copy(sent, sent, lane_send).wait()
    for _ in range(1, quads):
        pltpu.make_async_copy(stage, stage, far_send).wait()
    sent = toks.at[pl.ds(0, x_rows), :]
    pltpu.make_async_copy(sent, sent, tx_send).wait()
    pltpu.make_async_copy(z_part(0), z_part(0), tz_send).wait()
    sent = toks.at[pl.ds(0, 2 * rows), :]
    pltpu.make_async_copy(sent, sent, pair_send).wait()


def store(p_in, m_in, h_in, p_out, m_out, hidden, p_sem, m_sem, h_sem):
    blocks, _, width = h_in.shape
    p_copy = pltpu.make_async_copy(p_in, p_out, p_sem)
    m_copy = pltpu.make_async_copy(m_in, m_out, m_sem)
    for j in range(blocks):
        pltpu.make_async_copy(h_in.at[j], hidden.at[:, pl.ds(j * width, width)], h_sem).start()
    p_copy.start()
    m_copy.start()
    pltpu.make_async_copy(h_in, h_in, h_sem).wait()
    p_copy.wait()
    m_copy.wait()


def solution(mesh):
    groups, shards = mesh.shape["rep"], mesh.shape["fsdp"]

    def body(tokens, norm_gain, outer_params, momentum, deltas):
        rows, model = tokens.shape
        _, height, hid = outer_params.shape
        width = WIDTH
        chunks = hid // (LANES * width)
        pieces = chunks * LANES
        z_rows = rows // 4
        x_rows = rows - z_rows
        bf16, f32 = jnp.bfloat16, jnp.float32
        dma = pltpu.SemaphoreType.DMA
        strip = pltpu.VMEM((pieces, 2, height, width), bf16)
        anywhere = pl.BlockSpec(memory_space=pl.ANY)
        inside = pl.BlockSpec(memory_space=pltpu.VMEM)
        new_params, new_momentum, blocks = pl.pallas_call(
            functools.partial(kernel, groups, shards, z_rows),
            out_shape=(
                pltpu.VMEM(outer_params.shape, f32),
                pltpu.VMEM(outer_params.shape, f32),
                pltpu.VMEM((pieces, rows, width), bf16),
            ),
            in_specs=[anywhere, inside, anywhere, anywhere, anywhere],
            out_specs=(inside, inside, inside),
            scratch_shapes=[
                pltpu.VMEM((LANES * rows, model), bf16),
                pltpu.VMEM((chunks, model, 2 * width), bf16),
                pltpu.VMEM((pieces, height, 2 * width), bf16),
                strip, strip, strip,
                pltpu.VMEM((chunks, LANES - 1, x_rows, width), bf16),
                pltpu.VMEM((chunks, (LANES - 1) * z_rows, width), bf16),
                dma((pieces,)), dma((2,)), dma, dma,
                dma((pieces,)), dma((pieces,)), dma((pieces,)), dma, dma,
                dma((PARTS,)), dma, dma, dma, dma((2,)), dma((2,)), dma,
                dma((chunks, LANES)), dma, dma((chunks,)), dma, dma((2,)), dma((2,)),
            ],
            compiler_params=pltpu.CompilerParams(
                collective_id=0, has_side_effects=True, vmem_limit_bytes=175 * 256 * 1024),
            name="round",
        )(tokens, norm_gain.reshape(1, model), outer_params, momentum, deltas)
        return pl.pallas_call(
            store,
            out_shape=(
                jax.ShapeDtypeStruct(outer_params.shape, f32),
                jax.ShapeDtypeStruct(outer_params.shape, f32),
                jax.ShapeDtypeStruct((rows, hid), bf16),
            ),
            in_specs=[inside, inside, inside],
            out_specs=(anywhere, anywhere, anywhere),
            scratch_shapes=[dma, dma, dma],
            compiler_params=pltpu.CompilerParams(vmem_limit_bytes=22 * 1024 * 1024),
            name="store",
        )(new_params, new_momentum, blocks)

    in_specs = (
        P(("rep", "fsdp"), None),
        P(),
        P(None, "fsdp", None),
        P(None, "fsdp", None),
        P("rep", None, "fsdp", None),
    )
    out_specs = (P(None, "fsdp", None), P(None, "fsdp", None), P(("rep", "fsdp"), None))
    return jax.shard_map(body, mesh=mesh, in_specs=in_specs, out_specs=out_specs, check_vma=False)
```

```python
import functools
import math

import jax
import jax.numpy as jnp
from jax import lax
from jax.experimental import pallas as pl
from jax.experimental.pallas import tpu as pltpu
from jax.sharding import PartitionSpec as P

EPS = 1e-05
MU = 0.9
RATE = 0.7
CORES = 2
LANES = 4
WIDTH = 128
PARTS = 6
SEND_AT = ((None, None, None, None, 5, 9), (None, None, 3, 7, 11, 15))
PASS_AT = ((2, 4, 6, 8, 10, 13), (2, 4, 8, 12, 15, 19))
DOT_AT = (14, 20)
SUM_LAG = 1
STEP_LAG = 2
NEAR_LAG = 4
FAR_LAG = 5
DOT_LAG = 12


def advance(params, moment, summed, groups):
    outer_grad = summed * (1.0 / groups)
    moment_next = MU * moment + outer_grad
    params_next = params - RATE * (outer_grad + MU * moment_next)
    return (params_next, moment_next)


def other(bit, turned):
    return 1 - bit if turned else bit


def kernel(
    groups, shards, z_rows,
    tokens, gain, params, moment, deltas,
    p_out, m_out, hid_out,
    toks, weights, stage, own, peer_in, total, h_x, h_z,
    load_sem, token_sem, p_sem, m_sem,
    part_recv, peer_recv, total_recv, part_send, total_send,
    tx_recv, tx_send, tz_recv, tz_send, pair_recv, diag_recv, pair_send,
    lane_recv, lane_send, far_recv, far_send, h_recv, h_send,
):
    pieces, _, height, width = own.shape
    chunks = pieces // LANES
    rows, model = tokens.shape
    x_rows = rows - z_rows
    z_base = LANES * x_rows
    quarter = chunks * width
    quads = shards // LANES
    bf16, f32 = jnp.bfloat16, jnp.float32
    rep = lax.axis_index("rep")
    mine = lax.axis_index("fsdp")
    core = mine % CORES
    chip = mine // CORES
    x_bit = chip % 2
    quad = chip // 2
    turn = ((rep + 1) // 2) % 2
    lane = ((x_bit + turn) % 2) * 2 + core
    middle = groups // 2
    low = rep < middle
    inward = jnp.where(low, rep + 1, rep - 1)
    outward = jnp.where(low, rep - 1, rep + 1)
    at_end = (rep == 0) | (rep == groups - 1)
    at_middle = (rep == middle - 1) | (rep == middle)
    z_pair = rep + 1 - 2 * (rep % 2)

    def shard(bit, which_core, where=quad):
        return (where * 2 + bit) * CORES + which_core

    def at_x(k):
        return shard(other(x_bit, k // 2), other(core, k % 2))

    def remote(src, dst, send, recv, **device):
        return pltpu.make_async_remote_copy(
            src_ref=src, dst_ref=dst, send_sem=send, recv_sem=recv,
            device_id=device, device_id_type=pl.DeviceIdType.MESH)

    def z_device(k):
        near = {"fsdp": chip * CORES + other(core, k % 2)}
        return {"rep": z_pair, **near} if k // 2 else near

    def order(c, i):
        return jnp.where(c < chunks // 2, i, LANES - 1 - i)

    def columns(c, i):
        at = order(c, i)
        h = (x_bit + at // 2) % 2 * 2 + (core + at % 2) % 2
        return pl.ds(pl.multiple_of(h * quarter + c * width, width), width)

    def relative(c, i):
        at = order(c, i)
        return (at // 2 + turn) % 2, at % 2

    def lane_shard(c, i):
        far, near = relative(c, i)
        return shard((x_bit + far) % 2, (core + near) % 2)

    def block(c, owner):
        return weights.at[c, pl.ds(pl.multiple_of(owner * height, height), height), :]

    def delta_load(c, i):
        n = c * LANES + i
        return pltpu.make_async_copy(deltas.at[0, :, :, columns(c, i)], own.at[n], load_sem.at[n])

    def part_copy(dst, n, recv):
        return remote(own.at[n], dst.at[n], part_send, recv.at[n], rep=inward)

    def total_copy(n):
        return remote(total.at[n], total.at[n], total_send, total_recv.at[n], rep=outward)

    def lane_copy(c, i):
        return remote(stage.at[c * LANES + i], block(c, mine), lane_send, lane_recv.at[c, i], fsdp=lane_shard(c, i))

    def far_copy(c, i, r):
        at = block(c, lane_shard(c, i))
        return remote(at, at, far_send, far_recv.at[c], fsdp=shard(x_bit, core, (quad + r) % quads))

    part_rows = x_rows // PARTS

    def x_part(k, j):
        return toks.at[pl.ds(k * x_rows + j * part_rows, part_rows), :]

    def z_part(k, half=None):
        if half is None:
            return toks.at[pl.ds(z_base + k * z_rows, z_rows), :]
        return toks.at[pl.ds(z_base + k * z_rows + half * (z_rows // 2), z_rows // 2), :]

    def token_x(j):
        return remote(x_part(0, j), x_part(2, j), tx_send, tx_recv.at[j], fsdp=at_x(2))

    def token_pass(j):
        return remote(x_part(2, j), x_part(3, j), pair_send, diag_recv.at[0], fsdp=at_x(1))

    def token_z(half):
        return remote(z_part(0, half), z_part(2, half), tz_send, tz_recv, rep=z_pair)

    def token_z_pass():
        return remote(z_part(2), z_part(3), pair_send, diag_recv.at[1], fsdp=at_x(1))

    @pl.loop(0, chunks)
    def _(c):
        for i in range(LANES):
            delta_load(c, i).start()

    token_copies = [
        pltpu.make_async_copy(
            tokens.at[pl.ds(j * part_rows, part_rows), :], x_part(0, j), token_sem.at[j])
        for j in range(PARTS)
    ]
    token_copies.append(pltpu.make_async_copy(tokens.at[pl.ds(x_rows, z_rows), :], z_part(0), token_sem.at[PARTS]))
    for copy in token_copies:
        copy.start()
    p_load = pltpu.make_async_copy(params, p_out, p_sem)
    m_load = pltpu.make_async_copy(moment, m_out, m_sem)
    p_load.start()
    m_load.start()

    barrier = pltpu.get_barrier_semaphore()
    greeted = 0
    for k in (1, 2, 3):
        pl.semaphore_signal(barrier, inc=1, device_id={"fsdp": at_x(k)}, device_id_type=pl.DeviceIdType.MESH)
    for r in range(1, quads):
        pl.semaphore_signal(
            barrier, inc=1, device_id={"fsdp": shard(x_bit, core, (quad + r) % quads)}, device_id_type=pl.DeviceIdType.MESH)
    pl.semaphore_signal(barrier, inc=1, device_id=z_device(3), device_id_type=pl.DeviceIdType.MESH)
    pl.semaphore_signal(barrier, inc=1, device_id={"rep": inward}, device_id_type=pl.DeviceIdType.MESH)
    greeted = LANES - 1 + quads - 1 + 2

    @pl.when(jnp.logical_not(at_end))
    def _():
        pl.semaphore_signal(barrier, inc=1, device_id={"rep": outward}, device_id_type=pl.DeviceIdType.MESH)

    @pl.when(jnp.logical_not(at_end))
    def _():
        pl.semaphore_wait(barrier, greeted + 1)

    @pl.when(at_end)
    def _():
        pl.semaphore_wait(barrier, greeted)

    @pl.loop(0, pieces)
    def _(n):
        pltpu.make_async_copy(own.at[n], own.at[n], load_sem.at[n]).wait()

        @pl.when(at_end & jnp.logical_not(at_middle))
        def _():
            part_copy(total, n, part_recv).start()

        @pl.when(at_end & at_middle)
        def _():
            part_copy(peer_in, n, peer_recv).start()

    piece = 32

    def normalize(first, count):
        @pl.loop(0, count // piece)
        def _(i):
            at = pl.ds(pl.multiple_of(first + i * piece, piece), piece)
            values = toks[at, :].astype(f32)
            scale = lax.rsqrt(jnp.mean(values * values, axis=-1, keepdims=True) + EPS)
            toks[at, :] = (values * scale * gain[...]).astype(bf16)

    for j in range(PARTS):
        token_copies[j].wait()
        normalize(j * part_rows, part_rows)
        early = [role[j] is None for role in SEND_AT]
        if all(early):
            token_x(j).start()
        elif any(early):
            @pl.when(at_end if early[0] else jnp.logical_not(at_end))
            def _(j=j):
                token_x(j).start()

    token_copies[PARTS].wait()
    normalize(z_base, z_rows)
    token_z(0).start()

    @pl.when(at_end)
    def _():
        token_z(1).start()

    remote(toks.at[pl.ds(0, x_rows), :], toks.at[pl.ds(x_rows, x_rows), :], pair_send, pair_recv.at[0], fsdp=at_x(1)).start()
    remote(z_part(0), z_part(1), pair_send, pair_recv.at[1], fsdp=at_x(1)).start()

    factor = 1.0 / math.sqrt(model)

    def gated(at, c):
        both = jnp.dot(toks[at, :], weights[c], preferred_element_type=f32) * factor
        gate, up = both[:, :width], both[:, width:]
        return (gate / (1.0 + jnp.exp(-gate)) * up).astype(bf16)

    def live(c):
        return (c >= 0) & (c < chunks)

    def shifted(t, i, lag):
        return t + (i - lag) // LANES, (i - lag) % LANES

    def gather_in(c, i):
        n = c * LANES + i
        part_copy(total, n, part_recv).wait_recv()
        own[n] = (own[n].astype(f32) + total[n].astype(f32)).astype(bf16)

        @pl.when(at_middle)
        def _():
            part_copy(peer_in, n, peer_recv).start()

        @pl.when(jnp.logical_not(at_middle))
        def _():
            part_copy(total, n, part_recv).start()

    def join(c, i):
        n = c * LANES + i
        part_copy(peer_in, n, peer_recv).wait_recv()
        total[n] = (own[n].astype(f32) + peer_in[n].astype(f32)).astype(bf16)

        @pl.when(jnp.logical_not(at_end))
        def _():
            total_copy(n).start()

    def update(c, i):
        n = c * LANES + i

        @pl.when(jnp.logical_not(at_middle))
        def _():
            total_copy(n).wait_recv()

            @pl.when(jnp.logical_not(at_end))
            def _():
                total_copy(n).start()

        if i == 0:
            @pl.when(c == 0)
            def _():
                p_load.wait()
                m_load.wait()

        at = columns(c, i)
        far, near = relative(c, i)
        kept = (far == 0) & (near == 0)
        for which in range(2):
            stepped, moved = advance(p_out[which, :, at], m_out[which, :, at], total[n, which].astype(f32), groups)
            p_out[which, :, at] = stepped
            m_out[which, :, at] = moved
            stage[n, :, which * width:(which + 1) * width] = stepped.astype(bf16)

        @pl.when(jnp.logical_not(kept))
        def _():
            lane_copy(c, i).start()

        @pl.when(kept)
        def _():
            start = pl.multiple_of(mine * height, height)
            weights[c, pl.ds(start, height), :] = stage[n]
            for r in range(1, quads):
                far_copy(c, i, r).start()

    def pass_on(c, i, from_far):
        far, near = relative(c, i)

        @pl.when((far == 1) if from_far else (far == 0) & (near == 1))
        def _():
            lane_copy(c, i).wait_recv()
            for r in range(1, quads):
                far_copy(c, i, r).start()

    def pass_near(c, i):
        pass_on(c, i, False)

    def pass_far(c, i):
        pass_on(c, i, True)

    def project(unit):
        c, k = unit // LANES, LANES - 1 - unit % LANES

        @pl.when(unit == 0)
        def _():
            there = toks.at[pl.ds(x_rows, x_rows), :]
            pltpu.make_async_copy(there, there, pair_recv.at[0]).wait()
            pltpu.make_async_copy(there, there, diag_recv.at[0]).wait()

        @pl.when(k == LANES - 1)
        def _():
            for _ in range(1, quads):
                arrived = weights.at[c, pl.ds(0, LANES * height), :]
                pltpu.make_async_copy(arrived, arrived, far_recv.at[c]).wait()

        h_x[c, k] = gated(pl.ds(pl.multiple_of(k * x_rows, x_rows), x_rows), c)
        slot = lane * chunks + c

        @pl.when(k == 0)
        def _():
            hid_out[slot, 0:x_rows, :] = h_x[c, 0]

        @pl.when(k > 0)
        def _():
            owner = shard((x_bit + k // 2) % 2, (core + k % 2) % 2)
            remote(h_x.at[c, k], hid_out.at[slot, pl.ds(0, x_rows), :], h_send.at[0], h_recv.at[0], fsdp=owner).start()

    def project_z(c):
        hidden = gated(slice(z_base, z_base + LANES * z_rows), c)
        slot = lane * chunks + c
        hid_out[slot, x_rows:rows, :] = hidden[0:z_rows]
        h_z[c] = hidden[z_rows:]
        for k in (3, 2, 1):
            remote(h_z.at[c, pl.ds((k - 1) * z_rows, z_rows), :], hid_out.at[slot, pl.ds(x_rows, z_rows), :],
                   h_send.at[1], h_recv.at[1], **z_device(k)).start()

    tail = -(-DOT_LAG // LANES)
    tail_z = -(-chunks // (tail - 1))
    dot_at = jnp.where(at_end, DOT_AT[0], DOT_AT[1])

    def dots_done(n):
        paced = jnp.maximum(n + 1 - dot_at, 0) * 4 // 3
        return jnp.clip(jnp.minimum(paced, n + 1 - DOT_LAG), 0, pieces)

    stages = (
        (gather_in, 0, jnp.logical_not(at_end)), (join, SUM_LAG, at_middle), (update, STEP_LAG, None),
        (pass_near, NEAR_LAG, None), (pass_far, FAR_LAG, None))

    @pl.loop(0, chunks + tail)
    def _(t):
        for i in range(LANES):
            for stepper, lag, when in stages:
                c, at = shifted(t, i, lag)

                @pl.when(live(c) if when is None else live(c) & when)
                def _(stepper=stepper, c=c, at=at):
                    stepper(c, at)

            for role, here in enumerate((at_end, jnp.logical_not(at_end))):
                for j in range(PARTS):
                    if SEND_AT[role][j] is not None and SEND_AT[role][j] % LANES == i:
                        @pl.when((t == SEND_AT[role][j] // LANES) & here)
                        def _(j=j):
                            token_x(j).start()

                    if PASS_AT[role][j] % LANES == i:
                        @pl.when((t == PASS_AT[role][j] // LANES) & here)
                        def _(j=j):
                            token_x(j).wait_recv()
                            token_pass(j).start()

            n = t * LANES + i

            @pl.loop(dots_done(n - 1), dots_done(n))
            def _(unit):
                project(unit)

            if i == (SUM_LAG + 1) % LANES:
                @pl.when((t == chunks + (SUM_LAG + 1) // LANES) & jnp.logical_not(at_end))
                def _():
                    token_z(1).start()

        @pl.when(t == chunks)
        def _():
            pltpu.make_async_copy(z_part(2), z_part(2), tz_recv).wait()
            token_z_pass().start()

        @pl.when(t == chunks + 1)
        def _():
            pltpu.make_async_copy(z_part(1), z_part(1), pair_recv.at[1]).wait()
            pltpu.make_async_copy(z_part(3), z_part(3), diag_recv.at[1]).wait()

        @pl.when(t > chunks)
        def _():
            first = (t - chunks - 1) * tail_z

            @pl.loop(first, jnp.minimum(first + tail_z, chunks))
            def _(c):
                project_z(c)

    got = hid_out.at[pl.ds(0, (LANES - 1) * chunks), pl.ds(0, x_rows), :]
    pltpu.make_async_copy(got, got, h_recv.at[0]).wait()
    got = hid_out.at[pl.ds(0, (LANES - 1) * chunks), pl.ds(x_rows, z_rows), :]
    pltpu.make_async_copy(got, got, h_recv.at[1]).wait()
    sent = h_x.at[:, pl.ds(1, LANES - 1)]
    pltpu.make_async_copy(sent, sent, h_send.at[0]).wait()
    pltpu.make_async_copy(h_z, h_z, h_send.at[1]).wait()
    pltpu.make_async_copy(own, own, part_send).wait()

    @pl.when(jnp.logical_not(at_end))
    def _():
        pltpu.make_async_copy(total, total, total_send).wait()

    sent = stage.at[pl.ds(0, (LANES - 1) * chunks)]
    pltpu.make_async_copy(sent, sent, lane_send).wait()
    for _ in range(1, quads):
        pltpu.make_async_copy(stage, stage, far_send).wait()
    sent = toks.at[pl.ds(0, x_rows), :]
    pltpu.make_async_copy(sent, sent, tx_send).wait()
    pltpu.make_async_copy(z_part(0), z_part(0), tz_send).wait()
    sent = toks.at[pl.ds(0, 2 * rows), :]
    pltpu.make_async_copy(sent, sent, pair_send).wait()


def store(p_in, m_in, h_in, p_out, m_out, hidden, p_sem, m_sem, h_sem):
    blocks, _, width = h_in.shape
    p_copy = pltpu.make_async_copy(p_in, p_out, p_sem)
    m_copy = pltpu.make_async_copy(m_in, m_out, m_sem)
    for j in range(blocks):
        pltpu.make_async_copy(h_in.at[j], hidden.at[:, pl.ds(j * width, width)], h_sem).start()
    p_copy.start()
    m_copy.start()
    pltpu.make_async_copy(h_in, h_in, h_sem).wait()
    p_copy.wait()
    m_copy.wait()


def solution(mesh):
    groups, shards = mesh.shape["rep"], mesh.shape["fsdp"]

    def body(tokens, norm_gain, outer_params, momentum, deltas):
        rows, model = tokens.shape
        _, height, hid = outer_params.shape
        width = WIDTH
        chunks = hid // (LANES * width)
        pieces = chunks * LANES
        z_rows = rows // 4
        x_rows = rows - z_rows
        bf16, f32 = jnp.bfloat16, jnp.float32
        dma = pltpu.SemaphoreType.DMA
        strip = pltpu.VMEM((pieces, 2, height, width), bf16)
        anywhere = pl.BlockSpec(memory_space=pl.ANY)
        inside = pl.BlockSpec(memory_space=pltpu.VMEM)
        new_params, new_momentum, blocks = pl.pallas_call(
            functools.partial(kernel, groups, shards, z_rows),
            out_shape=(
                pltpu.VMEM(outer_params.shape, f32),
                pltpu.VMEM(outer_params.shape, f32),
                pltpu.VMEM((pieces, rows, width), bf16),
            ),
            in_specs=[anywhere, inside, anywhere, anywhere, anywhere],
            out_specs=(inside, inside, inside),
            scratch_shapes=[
                pltpu.VMEM((LANES * rows, model), bf16),
                pltpu.VMEM((chunks, model, 2 * width), bf16),
                pltpu.VMEM((pieces, height, 2 * width), bf16),
                strip, strip, strip,
                pltpu.VMEM((chunks, LANES, x_rows, width), bf16),
                pltpu.VMEM((chunks, (LANES - 1) * z_rows, width), bf16),
                dma((pieces,)), dma((PARTS + 1,)), dma, dma,
                dma((pieces,)), dma((pieces,)), dma((pieces,)), dma, dma,
                dma((PARTS,)), dma, dma, dma, dma((2,)), dma((2,)), dma,
                dma((chunks, LANES)), dma, dma((chunks,)), dma, dma((2,)), dma((2,)),
            ],
            compiler_params=pltpu.CompilerParams(
                collective_id=0, has_side_effects=True, vmem_limit_bytes=175 * 256 * 1024),
            name="round",
        )(tokens, norm_gain.reshape(1, model), outer_params, momentum, deltas)
        return pl.pallas_call(
            store,
            out_shape=(
                jax.ShapeDtypeStruct(outer_params.shape, f32),
                jax.ShapeDtypeStruct(outer_params.shape, f32),
                jax.ShapeDtypeStruct((rows, hid), bf16),
            ),
            in_specs=[inside, inside, inside],
            out_specs=(anywhere, anywhere, anywhere),
            scratch_shapes=[dma, dma, dma],
            compiler_params=pltpu.CompilerParams(vmem_limit_bytes=22 * 1024 * 1024),
            name="store",
        )(new_params, new_momentum, blocks)

    in_specs = (
        P(("rep", "fsdp"), None),
        P(),
        P(None, "fsdp", None),
        P(None, "fsdp", None),
        P("rep", None, "fsdp", None),
    )
    out_specs = (P(None, "fsdp", None), P(None, "fsdp", None), P(("rep", "fsdp"), None))
    return jax.shard_map(body, mesh=mesh, in_specs=in_specs, out_specs=out_specs, check_vma=False)
```

```python
import functools
import math

import jax
import jax.numpy as jnp
from jax import lax
from jax.experimental import pallas as pl
from jax.experimental.pallas import tpu as pltpu
from jax.sharding import PartitionSpec as P

EPS = 1e-05
MU = 0.9
RATE = 0.7
CORES = 2
LANES = 4
WIDTH = 128
PARTS = 6
SEND_AT = ((None, None, None, None, 4, 8), (None, None, 2, 6, 10, 14))
PASS_AT = ((2, 4, 6, 8, 10, 14), (2, 4, 8, 12, 16, 19))
DOT_AT = (15, 20)
Z_PARTS = 4
Z_EARLY = 2
SUM_LAG = 1
NEAR_LAG = 3
FAR_LAG = 5
DOT_LAG = (10, 12)


def advance(params, moment, summed, groups):
    outer_grad = summed * (1.0 / groups)
    moment_next = MU * moment + outer_grad
    params_next = params - RATE * (outer_grad + MU * moment_next)
    return (params_next, moment_next)


def other(bit, turned):
    return 1 - bit if turned else bit


def kernel(
    groups, shards, z_rows,
    tokens, gain, params, moment, deltas,
    p_out, m_out, hid_out,
    toks, weights, stage, own, peer_in, total, h_x, h_z,
    load_sem, token_sem, p_sem, m_sem,
    part_recv, peer_recv, total_recv, part_send, total_send,
    tx_recv, tx_send, tz_recv, tz_send, pair_recv, diag_recv, pair_send,
    lane_recv, lane_send, far_recv, far_send, h_recv, h_send,
):
    pieces, _, height, width = own.shape
    chunks = pieces // LANES
    rows, model = tokens.shape
    x_rows = rows - z_rows
    z_base = LANES * x_rows
    quarter = chunks * width
    quads = shards // LANES
    bf16, f32 = jnp.bfloat16, jnp.float32
    rep = lax.axis_index("rep")
    mine = lax.axis_index("fsdp")
    core = mine % CORES
    chip = mine // CORES
    x_bit = chip % 2
    quad = chip // 2
    turn = ((rep + 1) // 2) % 2
    lane = ((x_bit + turn) % 2) * 2 + core
    middle = groups // 2
    low = rep < middle
    inward = jnp.where(low, rep + 1, rep - 1)
    outward = jnp.where(low, rep - 1, rep + 1)
    at_end = (rep == 0) | (rep == groups - 1)
    at_middle = (rep == middle - 1) | (rep == middle)
    z_pair = rep + 1 - 2 * (rep % 2)

    def shard(bit, which_core, where=quad):
        return (where * 2 + bit) * CORES + which_core

    def at_x(k):
        return shard(other(x_bit, k // 2), other(core, k % 2))

    def remote(src, dst, send, recv, **device):
        return pltpu.make_async_remote_copy(
            src_ref=src, dst_ref=dst, send_sem=send, recv_sem=recv,
            device_id=device, device_id_type=pl.DeviceIdType.MESH)

    def z_device(k):
        near = {"fsdp": chip * CORES + other(core, k % 2)}
        return {"rep": z_pair, **near} if k // 2 else near

    def order(c, i):
        return jnp.where(c < chunks // 2, i, LANES - 1 - i)

    def columns(c, i):
        at = order(c, i)
        h = (x_bit + at // 2) % 2 * 2 + (core + at % 2) % 2
        return pl.ds(pl.multiple_of(h * quarter + c * width, width), width)

    def relative(c, i):
        at = order(c, i)
        return (at // 2 + turn) % 2, at % 2

    def lane_shard(c, i):
        far, near = relative(c, i)
        return shard((x_bit + far) % 2, (core + near) % 2)

    def block(c, owner):
        return weights.at[c, pl.ds(pl.multiple_of(owner * height, height), height), :]

    def delta_load(c, i):
        n = c * LANES + i
        return pltpu.make_async_copy(deltas.at[0, :, :, columns(c, i)], own.at[n], load_sem.at[n])

    def part_copy(dst, n, recv):
        return remote(own.at[n], dst.at[n], part_send, recv.at[n], rep=inward)

    def total_copy(n):
        return remote(total.at[n], total.at[n], total_send, total_recv.at[n], rep=outward)

    def lane_copy(c, i):
        return remote(stage.at[c * LANES + i], block(c, mine), lane_send, lane_recv.at[c, i], fsdp=lane_shard(c, i))

    def far_copy(c, i, r):
        at = block(c, lane_shard(c, i))
        return remote(at, at, far_send, far_recv.at[c], fsdp=shard(x_bit, core, (quad + r) % quads))

    part_rows = x_rows // PARTS

    def x_part(k, j):
        return toks.at[pl.ds(k * x_rows + j * part_rows, part_rows), :]

    def z_part(k, j=None):
        if j is None:
            return toks.at[pl.ds(z_base + k * z_rows, z_rows), :]
        return toks.at[pl.ds(z_base + k * z_rows + j * (z_rows // Z_PARTS), z_rows // Z_PARTS), :]

    def token_x(j):
        return remote(x_part(0, j), x_part(2, j), tx_send, tx_recv.at[j], fsdp=at_x(2))

    def token_pass(j):
        return remote(x_part(2, j), x_part(3, j), pair_send, diag_recv.at[0], fsdp=at_x(1))

    def token_z(j):
        return remote(z_part(0, j), z_part(2, j), tz_send, tz_recv, rep=z_pair)

    def token_z_pass():
        return remote(z_part(2), z_part(3), pair_send, diag_recv.at[1], fsdp=at_x(1))

    @pl.loop(0, chunks)
    def _(c):
        for i in range(LANES):
            delta_load(c, i).start()

    token_copies = [
        pltpu.make_async_copy(
            tokens.at[pl.ds(j * part_rows, part_rows), :], x_part(0, j), token_sem.at[j])
        for j in range(PARTS)
    ]
    token_copies.append(pltpu.make_async_copy(tokens.at[pl.ds(x_rows, z_rows), :], z_part(0), token_sem.at[PARTS]))
    for copy in token_copies:
        copy.start()
    p_load = pltpu.make_async_copy(params, p_out, p_sem)
    m_load = pltpu.make_async_copy(moment, m_out, m_sem)
    p_load.start()
    m_load.start()

    barrier = pltpu.get_barrier_semaphore()
    greeted = 0
    for k in (1, 2, 3):
        pl.semaphore_signal(barrier, inc=1, device_id={"fsdp": at_x(k)}, device_id_type=pl.DeviceIdType.MESH)
    for r in range(1, quads):
        pl.semaphore_signal(
            barrier, inc=1, device_id={"fsdp": shard(x_bit, core, (quad + r) % quads)}, device_id_type=pl.DeviceIdType.MESH)
    pl.semaphore_signal(barrier, inc=1, device_id=z_device(3), device_id_type=pl.DeviceIdType.MESH)
    pl.semaphore_signal(barrier, inc=1, device_id={"rep": inward}, device_id_type=pl.DeviceIdType.MESH)
    greeted = LANES - 1 + quads - 1 + 2

    @pl.when(jnp.logical_not(at_end))
    def _():
        pl.semaphore_signal(barrier, inc=1, device_id={"rep": outward}, device_id_type=pl.DeviceIdType.MESH)

    @pl.when(jnp.logical_not(at_end))
    def _():
        pl.semaphore_wait(barrier, greeted + 1)

    @pl.when(at_end)
    def _():
        pl.semaphore_wait(barrier, greeted)

    @pl.loop(0, pieces)
    def _(n):
        pltpu.make_async_copy(own.at[n], own.at[n], load_sem.at[n]).wait()

        @pl.when(at_end & jnp.logical_not(at_middle))
        def _():
            part_copy(total, n, part_recv).start()

        @pl.when(at_end & at_middle)
        def _():
            part_copy(peer_in, n, peer_recv).start()

    piece = 32

    def normalize(first, count):
        @pl.loop(0, count // piece)
        def _(i):
            at = pl.ds(pl.multiple_of(first + i * piece, piece), piece)
            values = toks[at, :].astype(f32)
            scale = lax.rsqrt(jnp.mean(values * values, axis=-1, keepdims=True) + EPS)
            toks[at, :] = (values * scale * gain[...]).astype(bf16)

    for j in range(PARTS):
        token_copies[j].wait()
        normalize(j * part_rows, part_rows)
        early = [role[j] is None for role in SEND_AT]
        if all(early):
            token_x(j).start()
        elif any(early):
            @pl.when(at_end if early[0] else jnp.logical_not(at_end))
            def _(j=j):
                token_x(j).start()

    token_copies[PARTS].wait()
    normalize(z_base, z_rows)
    for j in range(Z_EARLY):
        token_z(j).start()

    @pl.when(at_end)
    def _():
        for j in range(Z_EARLY, Z_PARTS):
            token_z(j).start()

    remote(toks.at[pl.ds(0, x_rows), :], toks.at[pl.ds(x_rows, x_rows), :], pair_send, pair_recv.at[0], fsdp=at_x(1)).start()
    remote(z_part(0), z_part(1), pair_send, pair_recv.at[1], fsdp=at_x(1)).start()

    factor = 1.0 / math.sqrt(model)

    def gated(at, c):
        both = jnp.dot(toks[at, :], weights[c], preferred_element_type=f32) * factor
        gate, up = both[:, :width], both[:, width:]
        return (gate / (1.0 + jnp.exp(-gate)) * up).astype(bf16)

    def live(c):
        return (c >= 0) & (c < chunks)

    def shifted(t, i, lag):
        return t + (i - lag) // LANES, (i - lag) % LANES

    def gather_in(c, i):
        n = c * LANES + i
        part_copy(total, n, part_recv).wait_recv()
        own[n] = (own[n].astype(f32) + total[n].astype(f32)).astype(bf16)

        @pl.when(at_middle)
        def _():
            part_copy(peer_in, n, peer_recv).start()

        @pl.when(jnp.logical_not(at_middle))
        def _():
            part_copy(total, n, part_recv).start()

    def join(c, i):
        n = c * LANES + i
        part_copy(peer_in, n, peer_recv).wait_recv()
        total[n] = (own[n].astype(f32) + peer_in[n].astype(f32)).astype(bf16)

        @pl.when(jnp.logical_not(at_end))
        def _():
            total_copy(n).start()

    def update(c, i):
        n = c * LANES + i

        @pl.when(jnp.logical_not(at_middle))
        def _():
            total_copy(n).wait_recv()

            @pl.when(jnp.logical_not(at_end))
            def _():
                total_copy(n).start()

        if i == 0:
            @pl.when(c == 0)
            def _():
                p_load.wait()
                m_load.wait()

        at = columns(c, i)
        far, near = relative(c, i)
        kept = (far == 0) & (near == 0)
        for which in range(2):
            stepped, moved = advance(p_out[which, :, at], m_out[which, :, at], total[n, which].astype(f32), groups)
            p_out[which, :, at] = stepped
            m_out[which, :, at] = moved
            stage[n, :, which * width:(which + 1) * width] = stepped.astype(bf16)

        @pl.when(jnp.logical_not(kept))
        def _():
            lane_copy(c, i).start()

        @pl.when(kept)
        def _():
            start = pl.multiple_of(mine * height, height)
            weights[c, pl.ds(start, height), :] = stage[n]
            for r in range(1, quads):
                far_copy(c, i, r).start()

    def pass_on(c, i, from_far):
        far, near = relative(c, i)

        @pl.when((far == 1) if from_far else (far == 0) & (near == 1))
        def _():
            lane_copy(c, i).wait_recv()
            for r in range(1, quads):
                far_copy(c, i, r).start()

    def pass_near(c, i):
        pass_on(c, i, False)

    def pass_far(c, i):
        pass_on(c, i, True)

    def project(unit):
        c, k = unit // LANES, LANES - 1 - unit % LANES

        @pl.when(unit == 0)
        def _():
            there = toks.at[pl.ds(x_rows, x_rows), :]
            pltpu.make_async_copy(there, there, pair_recv.at[0]).wait()
            pltpu.make_async_copy(there, there, diag_recv.at[0]).wait()
            pltpu.make_async_copy(z_part(1), z_part(1), pair_recv.at[1]).wait()

        @pl.when(k == LANES - 1)
        def _():
            for _ in range(1, quads):
                arrived = weights.at[c, pl.ds(0, LANES * height), :]
                pltpu.make_async_copy(arrived, arrived, far_recv.at[c]).wait()

        h_x[c, k] = gated(pl.ds(pl.multiple_of(k * x_rows, x_rows), x_rows), c)
        slot = lane * chunks + c

        @pl.when(k == 0)
        def _():
            hid_out[slot, 0:x_rows, :] = h_x[c, 0]
            project_z_near(c)

        @pl.when(k > 0)
        def _():
            owner = shard((x_bit + k // 2) % 2, (core + k % 2) % 2)
            remote(h_x.at[c, k], hid_out.at[slot, pl.ds(0, x_rows), :], h_send.at[0], h_recv.at[0], fsdp=owner).start()

    def send_z(c, k, slot):
        remote(h_z.at[c, k - 1], hid_out.at[slot, pl.ds(x_rows, z_rows), :], h_send.at[1], h_recv.at[1], **z_device(k)).start()

    def project_z_near(c):
        hidden = gated(slice(z_base, z_base + 2 * z_rows), c)
        slot = lane * chunks + c
        h_z[c, 0] = hidden[z_rows:]
        send_z(c, 1, slot)
        hid_out[slot, x_rows:rows, :] = hidden[0:z_rows]

    def project_z_far(c):
        hidden = gated(slice(z_base + 2 * z_rows, z_base + 4 * z_rows), c)
        slot = lane * chunks + c
        h_z[c, 1] = hidden[0:z_rows]
        h_z[c, 2] = hidden[z_rows:]
        send_z(c, 3, slot)
        send_z(c, 2, slot)

    tail = -(-max(DOT_LAG) // LANES)
    dot_at = jnp.where(at_end, DOT_AT[0], DOT_AT[1])
    dot_lag = jnp.where(at_end, DOT_LAG[0], DOT_LAG[1])

    def dots_done(n):
        paced = jnp.maximum(n + 1 - dot_at, 0) * 4 // 3
        return jnp.clip(jnp.minimum(paced, n + 1 - dot_lag), 0, pieces)

    def on_pieces(t, i, *stages):
        for stepper, lag, when in stages:
            c, at = shifted(t, i, lag)

            @pl.when(live(c) if when is None else live(c) & when)
            def _(stepper=stepper, c=c, at=at):
                stepper(c, at)

    def on_tokens(t, i, table, act):
        for here, steps in zip((at_end, jnp.logical_not(at_end)), table):
            for j, step in enumerate(steps):
                if step is not None and step % LANES == i:
                    @pl.when((t == step // LANES) & here)
                    def _(j=j):
                        act(j)

    def pass_token(j):
        token_x(j).wait_recv()
        token_pass(j).start()

    def send_token(j):
        token_x(j).start()

    @pl.loop(0, chunks + tail)
    def _(t):
        for i in range(LANES):
            n = t * LANES + i
            on_pieces(t, i, (gather_in, 0, jnp.logical_not(at_end)), (pass_near, NEAR_LAG, None), (pass_far, FAR_LAG, None))
            on_tokens(t, i, PASS_AT, pass_token)

            @pl.loop(dots_done(n - 1), dots_done(n))
            def _(unit):
                project(unit)

            on_pieces(t, i, (join, SUM_LAG, at_middle), (update, SUM_LAG, None))
            on_tokens(t, i, SEND_AT, send_token)

            if i == LANES - 2:
                @pl.when(t == chunks)
                def _():
                    pltpu.make_async_copy(z_part(2), z_part(2), tz_recv).wait()
                    token_z_pass().start()

            if i == SUM_LAG:
                @pl.when((t == chunks) & jnp.logical_not(at_end))
                def _():
                    for j in range(Z_EARLY, Z_PARTS):
                        token_z(j).start()

        bulk = jnp.where(at_end, chunks, chunks + 1)

        @pl.when(t == bulk)
        def _():
            pltpu.make_async_copy(z_part(3), z_part(3), diag_recv.at[1]).wait()

        final = chunks + tail - 1

        @pl.loop(jnp.where(t == final, chunks - 1, 0), jnp.where(t == bulk, chunks - 1, jnp.where(t == final, chunks, 0)))
        def _(c):
            project_z_far(c)

    got = hid_out.at[pl.ds(0, (LANES - 1) * chunks), pl.ds(0, x_rows), :]
    pltpu.make_async_copy(got, got, h_recv.at[0]).wait()
    got = hid_out.at[pl.ds(0, (LANES - 1) * chunks), pl.ds(x_rows, z_rows), :]
    pltpu.make_async_copy(got, got, h_recv.at[1]).wait()
    sent = h_x.at[:, pl.ds(1, LANES - 1)]
    pltpu.make_async_copy(sent, sent, h_send.at[0]).wait()
    pltpu.make_async_copy(h_z, h_z, h_send.at[1]).wait()
    pltpu.make_async_copy(own, own, part_send).wait()

    @pl.when(jnp.logical_not(at_end))
    def _():
        pltpu.make_async_copy(total, total, total_send).wait()

    sent = stage.at[pl.ds(0, (LANES - 1) * chunks)]
    pltpu.make_async_copy(sent, sent, lane_send).wait()
    for _ in range(1, quads):
        pltpu.make_async_copy(stage, stage, far_send).wait()
    sent = toks.at[pl.ds(0, x_rows), :]
    pltpu.make_async_copy(sent, sent, tx_send).wait()
    pltpu.make_async_copy(z_part(0), z_part(0), tz_send).wait()
    sent = toks.at[pl.ds(0, 2 * rows), :]
    pltpu.make_async_copy(sent, sent, pair_send).wait()


def store(p_in, m_in, h_in, p_out, m_out, hidden, p_sem, m_sem, h_sem):
    blocks, _, width = h_in.shape
    p_copy = pltpu.make_async_copy(p_in, p_out, p_sem)
    m_copy = pltpu.make_async_copy(m_in, m_out, m_sem)
    for j in range(blocks):
        pltpu.make_async_copy(h_in.at[j], hidden.at[:, pl.ds(j * width, width)], h_sem).start()
    p_copy.start()
    m_copy.start()
    pltpu.make_async_copy(h_in, h_in, h_sem).wait()
    p_copy.wait()
    m_copy.wait()


def solution(mesh):
    groups, shards = mesh.shape["rep"], mesh.shape["fsdp"]

    def body(tokens, norm_gain, outer_params, momentum, deltas):
        rows, model = tokens.shape
        _, height, hid = outer_params.shape
        width = WIDTH
        chunks = hid // (LANES * width)
        pieces = chunks * LANES
        z_rows = rows // 4
        x_rows = rows - z_rows
        bf16, f32 = jnp.bfloat16, jnp.float32
        dma = pltpu.SemaphoreType.DMA
        strip = pltpu.VMEM((pieces, 2, height, width), bf16)
        anywhere = pl.BlockSpec(memory_space=pl.ANY)
        inside = pl.BlockSpec(memory_space=pltpu.VMEM)
        new_params, new_momentum, blocks = pl.pallas_call(
            functools.partial(kernel, groups, shards, z_rows),
            out_shape=(
                pltpu.VMEM(outer_params.shape, f32),
                pltpu.VMEM(outer_params.shape, f32),
                pltpu.VMEM((pieces, rows, width), bf16),
            ),
            in_specs=[anywhere, inside, anywhere, anywhere, anywhere],
            out_specs=(inside, inside, inside),
            scratch_shapes=[
                pltpu.VMEM((LANES * rows, model), bf16),
                pltpu.VMEM((chunks, model, 2 * width), bf16),
                pltpu.VMEM((pieces, height, 2 * width), bf16),
                strip, strip, strip,
                pltpu.VMEM((chunks, LANES, x_rows, width), bf16),
                pltpu.VMEM((chunks, LANES - 1, z_rows, width), bf16),
                dma((pieces,)), dma((PARTS + 1,)), dma, dma,
                dma((pieces,)), dma((pieces,)), dma((pieces,)), dma, dma,
                dma((PARTS,)), dma, dma, dma, dma((2,)), dma((2,)), dma,
                dma((chunks, LANES)), dma, dma((chunks,)), dma, dma((2,)), dma((2,)),
            ],
            compiler_params=pltpu.CompilerParams(
                collective_id=0, has_side_effects=True, vmem_limit_bytes=175 * 256 * 1024),
            name="round",
        )(tokens, norm_gain.reshape(1, model), outer_params, momentum, deltas)
        return pl.pallas_call(
            store,
            out_shape=(
                jax.ShapeDtypeStruct(outer_params.shape, f32),
                jax.ShapeDtypeStruct(outer_params.shape, f32),
                jax.ShapeDtypeStruct((rows, hid), bf16),
            ),
            in_specs=[inside, inside, inside],
            out_specs=(anywhere, anywhere, anywhere),
            scratch_shapes=[dma, dma, dma],
            compiler_params=pltpu.CompilerParams(vmem_limit_bytes=22 * 1024 * 1024),
            name="store",
        )(new_params, new_momentum, blocks)

    in_specs = (
        P(("rep", "fsdp"), None),
        P(),
        P(None, "fsdp", None),
        P(None, "fsdp", None),
        P("rep", None, "fsdp", None),
    )
    out_specs = (P(None, "fsdp", None), P(None, "fsdp", None), P(("rep", "fsdp"), None))
    return jax.shard_map(body, mesh=mesh, in_specs=in_specs, out_specs=out_specs, check_vma=False)
```

```python
import functools
import math

import jax
import jax.numpy as jnp
from jax import lax
from jax.experimental import pallas as pl
from jax.experimental.pallas import tpu as pltpu
from jax.sharding import PartitionSpec as P

EPS = 1e-05
MU = 0.9
RATE = 0.7
CORES = 2
LANES = 4
WIDTH = 128
PARTS = 6
SEND_AT = ((None, None, None, None, 4, 8), (None, None, 2, 6, 10, 14))
PASS_AT = ((2, 4, 6, 8, 10, 14), (2, 4, 8, 12, 16, 19))
DOT_AT = (15, 20)
Z_PARTS = 4
Z_EARLY = 2
SUM_LAG = 1
NEAR_LAG = 3
FAR_LAG = (5, 6)
DOT_LAG = (10, 12)


def advance(params, moment, summed, groups):
    outer_grad = summed * (1.0 / groups)
    moment_next = MU * moment + outer_grad
    params_next = params - RATE * (outer_grad + MU * moment_next)
    return (params_next, moment_next)


def other(bit, turned):
    return 1 - bit if turned else bit


def kernel(
    groups, shards, z_rows,
    tokens, gain, params, moment, deltas,
    p_out, m_out, hid_out,
    toks, weights, stage, own, peer_in, total, h_x, h_z,
    load_sem, token_sem, p_sem, m_sem,
    part_recv, peer_recv, total_recv, part_send, total_send,
    tx_recv, tx_send, tz_recv, tz_send, pair_recv, diag_recv, pair_send,
    lane_recv, lane_send, far_recv, far_send, h_recv, h_send,
):
    pieces, _, height, width = own.shape
    chunks = pieces // LANES
    rows, model = tokens.shape
    x_rows = rows - z_rows
    z_base = LANES * x_rows
    quarter = chunks * width
    quads = shards // LANES
    bf16, f32 = jnp.bfloat16, jnp.float32
    rep = lax.axis_index("rep")
    mine = lax.axis_index("fsdp")
    core = mine % CORES
    chip = mine // CORES
    x_bit = chip % 2
    quad = chip // 2
    turn = ((rep + 1) // 2) % 2
    lane = ((x_bit + turn) % 2) * 2 + core
    middle = groups // 2
    low = rep < middle
    inward = jnp.where(low, rep + 1, rep - 1)
    outward = jnp.where(low, rep - 1, rep + 1)
    at_end = (rep == 0) | (rep == groups - 1)
    at_middle = (rep == middle - 1) | (rep == middle)
    z_pair = rep + 1 - 2 * (rep % 2)

    def shard(bit, which_core, where=quad):
        return (where * 2 + bit) * CORES + which_core

    def at_x(k):
        return shard(other(x_bit, k // 2), other(core, k % 2))

    def remote(src, dst, send, recv, **device):
        return pltpu.make_async_remote_copy(
            src_ref=src, dst_ref=dst, send_sem=send, recv_sem=recv,
            device_id=device, device_id_type=pl.DeviceIdType.MESH)

    def z_device(k):
        near = {"fsdp": chip * CORES + other(core, k % 2)}
        return {"rep": z_pair, **near} if k // 2 else near

    def order(c, i):
        return jnp.where(c < chunks // 2, i, LANES - 1 - i)

    def columns(c, i):
        at = order(c, i)
        h = (x_bit + at // 2) % 2 * 2 + (core + at % 2) % 2
        return pl.ds(pl.multiple_of(h * quarter + c * width, width), width)

    def relative(c, i):
        at = order(c, i)
        return (at // 2 + turn) % 2, at % 2

    def lane_shard(c, i):
        far, near = relative(c, i)
        return shard((x_bit + far) % 2, (core + near) % 2)

    def block(c, owner):
        return weights.at[c, pl.ds(pl.multiple_of(owner * height, height), height), :]

    def delta_load(c, i):
        n = c * LANES + i
        return pltpu.make_async_copy(deltas.at[0, :, :, columns(c, i)], own.at[n], load_sem.at[n])

    def part_copy(dst, n, recv):
        return remote(own.at[n], dst.at[n], part_send, recv.at[n], rep=inward)

    def total_copy(n):
        return remote(total.at[n], total.at[n], total_send, total_recv.at[n], rep=outward)

    def lane_copy(c, i):
        return remote(stage.at[c * LANES + i], block(c, mine), lane_send, lane_recv.at[c, i], fsdp=lane_shard(c, i))

    def far_copy(c, i, r):
        at = block(c, lane_shard(c, i))
        return remote(at, at, far_send, far_recv.at[c], fsdp=shard(x_bit, core, (quad + r) % quads))

    part_rows = x_rows // PARTS

    def x_part(k, j):
        return toks.at[pl.ds(k * x_rows + j * part_rows, part_rows), :]

    z_half = z_rows // 2
    z_quarter = z_rows // Z_PARTS
    far_base = z_base + 2 * z_rows

    def z_part(k):
        return toks.at[pl.ds(z_base + k * z_rows, z_rows), :]

    def z_far(k, h):
        return toks.at[pl.ds(far_base + h * z_rows + (k - 2) * z_half, z_half), :]

    def token_x(j):
        return remote(x_part(0, j), x_part(2, j), tx_send, tx_recv.at[j], fsdp=at_x(2))

    def token_pass(j):
        return remote(x_part(2, j), x_part(3, j), pair_send, diag_recv.at[0], fsdp=at_x(1))

    def token_z(j):
        h, within = j // (Z_PARTS // 2), j % (Z_PARTS // 2)
        src = toks.at[pl.ds(z_base + j * z_quarter, z_quarter), :]
        dst = toks.at[pl.ds(far_base + h * z_rows + within * z_quarter, z_quarter), :]
        return remote(src, dst, tz_send, tz_recv.at[h], rep=z_pair)

    def pass_z(h):
        pltpu.make_async_copy(z_far(2, h), z_far(2, h), tz_recv.at[h]).wait()
        remote(z_far(2, h), z_far(3, h), pair_send, diag_recv.at[1 + h], fsdp=at_x(1)).start()

    def passed_z(h):
        pltpu.make_async_copy(z_far(3, h), z_far(3, h), diag_recv.at[1 + h]).wait()

    barrier = pltpu.get_barrier_semaphore()
    for k in (1, 2, 3):
        pl.semaphore_signal(barrier, inc=1, device_id={"fsdp": at_x(k)}, device_id_type=pl.DeviceIdType.MESH)
    for r in range(1, quads):
        pl.semaphore_signal(
            barrier, inc=1, device_id={"fsdp": shard(x_bit, core, (quad + r) % quads)}, device_id_type=pl.DeviceIdType.MESH)
    pl.semaphore_signal(barrier, inc=1, device_id=z_device(3), device_id_type=pl.DeviceIdType.MESH)
    pl.semaphore_signal(barrier, inc=1, device_id={"rep": inward}, device_id_type=pl.DeviceIdType.MESH)
    greeted = LANES - 1 + quads - 1 + 2

    @pl.when(jnp.logical_not(at_end))
    def _():
        pl.semaphore_signal(barrier, inc=1, device_id={"rep": outward}, device_id_type=pl.DeviceIdType.MESH)

    @pl.loop(0, chunks)
    def _(c):
        for i in range(LANES):
            delta_load(c, i).start()

    token_copies = [
        pltpu.make_async_copy(
            tokens.at[pl.ds(j * part_rows, part_rows), :], x_part(0, j), token_sem.at[j])
        for j in range(PARTS)
    ]
    token_copies.append(pltpu.make_async_copy(tokens.at[pl.ds(x_rows, z_rows), :], z_part(0), token_sem.at[PARTS]))
    for copy in token_copies:
        copy.start()
    p_load = pltpu.make_async_copy(params, p_out, p_sem)
    m_load = pltpu.make_async_copy(moment, m_out, m_sem)
    p_load.start()
    m_load.start()

    @pl.when(jnp.logical_not(at_end))
    def _():
        pl.semaphore_wait(barrier, greeted + 1)

    @pl.when(at_end)
    def _():
        pl.semaphore_wait(barrier, greeted)

    @pl.loop(0, pieces)
    def _(n):
        pltpu.make_async_copy(own.at[n], own.at[n], load_sem.at[n]).wait()

        @pl.when(at_end & jnp.logical_not(at_middle))
        def _():
            part_copy(total, n, part_recv).start()

        @pl.when(at_end & at_middle)
        def _():
            part_copy(peer_in, n, peer_recv).start()

    piece = 32

    def normalize(first, count):
        @pl.loop(0, count // piece)
        def _(i):
            at = pl.ds(pl.multiple_of(first + i * piece, piece), piece)
            values = toks[at, :].astype(f32)
            scale = lax.rsqrt(jnp.mean(values * values, axis=-1, keepdims=True) + EPS)
            toks[at, :] = (values * scale * gain[...]).astype(bf16)

    for j in range(PARTS):
        token_copies[j].wait()
        normalize(j * part_rows, part_rows)
        early = [role[j] is None for role in SEND_AT]
        if all(early):
            token_x(j).start()
        elif any(early):
            @pl.when(at_end if early[0] else jnp.logical_not(at_end))
            def _(j=j):
                token_x(j).start()

    token_copies[PARTS].wait()
    normalize(z_base, z_rows)
    for j in range(Z_EARLY):
        token_z(j).start()

    @pl.when(at_end)
    def _():
        for j in range(Z_EARLY, Z_PARTS):
            token_z(j).start()

    remote(toks.at[pl.ds(0, x_rows), :], toks.at[pl.ds(x_rows, x_rows), :], pair_send, pair_recv.at[0], fsdp=at_x(1)).start()
    remote(z_part(0), z_part(1), pair_send, pair_recv.at[1], fsdp=at_x(1)).start()

    factor = 1.0 / math.sqrt(model)

    def gated(at, c):
        both = jnp.dot(toks[at, :], weights[c], preferred_element_type=f32) * factor
        gate, up = both[:, :width], both[:, width:]
        return (gate / (1.0 + jnp.exp(-gate)) * up).astype(bf16)

    def live(c):
        return (c >= 0) & (c < chunks)

    def shifted(t, i, lag):
        return t + (i - lag) // LANES, (i - lag) % LANES

    def gather_in(c, i):
        n = c * LANES + i
        part_copy(total, n, part_recv).wait_recv()
        own[n] = (own[n].astype(f32) + total[n].astype(f32)).astype(bf16)

        @pl.when(at_middle)
        def _():
            part_copy(peer_in, n, peer_recv).start()

        @pl.when(jnp.logical_not(at_middle))
        def _():
            part_copy(total, n, part_recv).start()

    def join(c, i):
        n = c * LANES + i
        part_copy(peer_in, n, peer_recv).wait_recv()
        total[n] = (own[n].astype(f32) + peer_in[n].astype(f32)).astype(bf16)

        @pl.when(jnp.logical_not(at_end))
        def _():
            total_copy(n).start()

    def update(c, i):
        n = c * LANES + i

        @pl.when(jnp.logical_not(at_middle))
        def _():
            total_copy(n).wait_recv()

            @pl.when(jnp.logical_not(at_end))
            def _():
                total_copy(n).start()

        if i == 0:
            @pl.when(c == 0)
            def _():
                p_load.wait()
                m_load.wait()

        at = columns(c, i)
        far, near = relative(c, i)
        kept = (far == 0) & (near == 0)
        for which in range(2):
            stepped, moved = advance(p_out[which, :, at], m_out[which, :, at], total[n, which].astype(f32), groups)
            p_out[which, :, at] = stepped
            m_out[which, :, at] = moved
            stage[n, :, which * width:(which + 1) * width] = stepped.astype(bf16)

        @pl.when(jnp.logical_not(kept))
        def _():
            lane_copy(c, i).start()

        @pl.when(kept)
        def _():
            start = pl.multiple_of(mine * height, height)
            weights[c, pl.ds(start, height), :] = stage[n]
            for r in range(1, quads):
                far_copy(c, i, r).start()

    def pass_on(c, i, from_far):
        far, near = relative(c, i)

        @pl.when((far == 1) if from_far else (far == 0) & (near == 1))
        def _():
            lane_copy(c, i).wait_recv()
            for r in range(1, quads):
                far_copy(c, i, r).start()

    def pass_near(c, i):
        pass_on(c, i, False)

    def pass_far(c, i):
        pass_on(c, i, True)

    def project(unit):
        c, k = unit // LANES, LANES - 1 - unit % LANES

        @pl.when(unit == 0)
        def _():
            there = toks.at[pl.ds(x_rows, x_rows), :]
            pltpu.make_async_copy(there, there, pair_recv.at[0]).wait()
            pltpu.make_async_copy(there, there, diag_recv.at[0]).wait()
            pltpu.make_async_copy(z_part(1), z_part(1), pair_recv.at[1]).wait()

            @pl.when(at_end)
            def _():
                passed_z(0)

        @pl.when(k == LANES - 1)
        def _():
            for _ in range(1, quads):
                arrived = weights.at[c, pl.ds(0, LANES * height), :]
                pltpu.make_async_copy(arrived, arrived, far_recv.at[c]).wait()

        h_x[c, k] = gated(pl.ds(pl.multiple_of(k * x_rows, x_rows), x_rows), c)
        slot = lane * chunks + c

        @pl.when(k == 0)
        def _():
            hid_out[slot, 0:x_rows, :] = h_x[c, 0]
            project_z_near(c)

            @pl.when(at_end)
            def _():
                project_z_far(c, 0)

        @pl.when(k > 0)
        def _():
            owner = shard((x_bit + k // 2) % 2, (core + k % 2) % 2)
            remote(h_x.at[c, k], hid_out.at[slot, pl.ds(0, x_rows), :], h_send.at[0], h_recv.at[0], fsdp=owner).start()

        @pl.when((c == chunks - 1) & (k == 2))
        def _():
            project_z_rest(c)

    def send_z(c, k, first, count):
        slot = lane * chunks + c
        remote(h_z.at[c, k - 1, pl.ds(first, count), :], hid_out.at[slot, pl.ds(x_rows + first, count), :],
               h_send.at[1], h_recv.at[1], **z_device(k)).start()

    def project_z_near(c):
        hidden = gated(slice(z_base, far_base), c)
        h_z[c, 0] = hidden[z_rows:]
        send_z(c, 1, 0, z_rows)
        hid_out[lane * chunks + c, x_rows:rows, :] = hidden[0:z_rows]

    def project_z_far(c, h):
        hidden = gated(slice(far_base + h * z_rows, far_base + (h + 1) * z_rows), c)
        at = slice(h * z_half, (h + 1) * z_half)
        h_z[c, 1, at, :] = hidden[0:z_half]
        h_z[c, 2, at, :] = hidden[z_half:]
        for k in (3, 2):
            send_z(c, k, h * z_half, z_half)

    def project_z_rest(c):
        @pl.when(jnp.logical_not(at_end))
        def _():
            project_z_far(c, 0)

        project_z_far(c, 1)

    tail = -(-max(DOT_LAG) // LANES)
    dot_at = jnp.where(at_end, DOT_AT[0], DOT_AT[1])
    dot_lag = jnp.where(at_end, DOT_LAG[0], DOT_LAG[1])

    def dots_done(n):
        paced = jnp.maximum(n + 1 - dot_at, 0) * 4 // 3
        return jnp.clip(jnp.minimum(paced, n + 1 - dot_lag), 0, pieces)

    def on_pieces(t, i, *stages):
        for stepper, lag, when in stages:
            c, at = shifted(t, i, lag)

            @pl.when(live(c) if when is None else live(c) & when)
            def _(stepper=stepper, c=c, at=at):
                stepper(c, at)

    def on_tokens(t, i, table, act):
        for here, steps in zip((at_end, jnp.logical_not(at_end)), table):
            for j, step in enumerate(steps):
                if step is not None and step % LANES == i:
                    @pl.when((t == step // LANES) & here)
                    def _(j=j):
                        act(j)

    def pass_token(j):
        token_x(j).wait_recv()
        token_pass(j).start()

    def send_token(j):
        token_x(j).start()

    @pl.loop(0, chunks + tail)
    def _(t):
        for i in range(LANES):
            n = t * LANES + i
            on_pieces(t, i, (gather_in, 0, jnp.logical_not(at_end)), (pass_near, NEAR_LAG, None), (pass_far, FAR_LAG[0], at_end), (pass_far, FAR_LAG[1], jnp.logical_not(at_end)))
            on_tokens(t, i, PASS_AT, pass_token)

            @pl.loop(dots_done(n - 1), dots_done(n))
            def _(unit):
                project(unit)

            on_pieces(t, i, (join, SUM_LAG, at_middle), (update, SUM_LAG, None))
            on_tokens(t, i, SEND_AT, send_token)

            if i == LANES - 1:
                @pl.when(t == jnp.where(at_end, 1, chunks))
                def _():
                    pass_z(0)

                @pl.when(t == chunks)
                def _():
                    pass_z(1)

            if i == SUM_LAG:
                @pl.when((t == chunks) & jnp.logical_not(at_end))
                def _():
                    for j in range(Z_EARLY, Z_PARTS):
                        token_z(j).start()

        @pl.when(t == jnp.where(at_end, chunks, chunks + 1))
        def _():
            @pl.when(jnp.logical_not(at_end))
            def _():
                passed_z(0)

            passed_z(1)

            @pl.loop(0, chunks - 1)
            def _(c):
                project_z_rest(c)

    got = hid_out.at[pl.ds(0, (LANES - 1) * chunks), pl.ds(0, x_rows), :]
    pltpu.make_async_copy(got, got, h_recv.at[0]).wait()
    got = hid_out.at[pl.ds(0, (LANES - 1) * chunks), pl.ds(x_rows, z_rows), :]
    pltpu.make_async_copy(got, got, h_recv.at[1]).wait()
    sent = h_x.at[:, pl.ds(1, LANES - 1)]
    pltpu.make_async_copy(sent, sent, h_send.at[0]).wait()
    pltpu.make_async_copy(h_z, h_z, h_send.at[1]).wait()
    pltpu.make_async_copy(own, own, part_send).wait()

    @pl.when(jnp.logical_not(at_end))
    def _():
        pltpu.make_async_copy(total, total, total_send).wait()

    sent = stage.at[pl.ds(0, (LANES - 1) * chunks)]
    pltpu.make_async_copy(sent, sent, lane_send).wait()
    for _ in range(1, quads):
        pltpu.make_async_copy(stage, stage, far_send).wait()
    sent = toks.at[pl.ds(0, x_rows), :]
    pltpu.make_async_copy(sent, sent, tx_send).wait()
    pltpu.make_async_copy(z_part(0), z_part(0), tz_send).wait()
    sent = toks.at[pl.ds(0, 2 * rows), :]
    pltpu.make_async_copy(sent, sent, pair_send).wait()


def store(p_in, m_in, h_in, p_out, m_out, hidden, p_sem, m_sem, h_sem):
    blocks, _, width = h_in.shape
    p_copy = pltpu.make_async_copy(p_in, p_out, p_sem)
    m_copy = pltpu.make_async_copy(m_in, m_out, m_sem)
    for j in range(blocks):
        pltpu.make_async_copy(h_in.at[j], hidden.at[:, pl.ds(j * width, width)], h_sem).start()
    for src, dst, sem in ((p_in, p_out, p_sem), (m_in, m_out, m_sem)):
        which, height, _ = src.shape
        for w in range(which):
            for r in range(4):
                at = pl.ds(r * (height // 4), height // 4)
                pltpu.make_async_copy(src.at[w, at], dst.at[w, at], sem).start()
    pltpu.make_async_copy(h_in, h_in, h_sem).wait()
    p_copy.wait()
    m_copy.wait()


def solution(mesh):
    groups, shards = mesh.shape["rep"], mesh.shape["fsdp"]

    def body(tokens, norm_gain, outer_params, momentum, deltas):
        rows, model = tokens.shape
        _, height, hid = outer_params.shape
        width = WIDTH
        chunks = hid // (LANES * width)
        pieces = chunks * LANES
        z_rows = rows // 4
        x_rows = rows - z_rows
        bf16, f32 = jnp.bfloat16, jnp.float32
        dma = pltpu.SemaphoreType.DMA
        strip = pltpu.VMEM((pieces, 2, height, width), bf16)
        anywhere = pl.BlockSpec(memory_space=pl.ANY)
        inside = pl.BlockSpec(memory_space=pltpu.VMEM)
        new_params, new_momentum, blocks = pl.pallas_call(
            functools.partial(kernel, groups, shards, z_rows),
            out_shape=(
                pltpu.VMEM(outer_params.shape, f32),
                pltpu.VMEM(outer_params.shape, f32),
                pltpu.VMEM((pieces, rows, width), bf16),
            ),
            in_specs=[anywhere, inside, anywhere, anywhere, anywhere],
            out_specs=(inside, inside, inside),
            scratch_shapes=[
                pltpu.VMEM((LANES * rows, model), bf16),
                pltpu.VMEM((chunks, model, 2 * width), bf16),
                pltpu.VMEM((pieces, height, 2 * width), bf16),
                strip, strip, strip,
                pltpu.VMEM((chunks, LANES, x_rows, width), bf16),
                pltpu.VMEM((chunks, LANES - 1, z_rows, width), bf16),
                dma((pieces,)), dma((PARTS + 1,)), dma, dma,
                dma((pieces,)), dma((pieces,)), dma((pieces,)), dma, dma,
                dma((PARTS,)), dma, dma((2,)), dma, dma((2,)), dma((3,)), dma,
                dma((chunks, LANES)), dma, dma((chunks,)), dma, dma((2,)), dma((2,)),
            ],
            compiler_params=pltpu.CompilerParams(
                collective_id=0, has_side_effects=True, vmem_limit_bytes=175 * 256 * 1024),
            name="round",
        )(tokens, norm_gain.reshape(1, model), outer_params, momentum, deltas)
        return pl.pallas_call(
            store,
            out_shape=(
                jax.ShapeDtypeStruct(outer_params.shape, f32),
                jax.ShapeDtypeStruct(outer_params.shape, f32),
                jax.ShapeDtypeStruct((rows, hid), bf16),
            ),
            in_specs=[inside, inside, inside],
            out_specs=(anywhere, anywhere, anywhere),
            scratch_shapes=[dma, dma, dma],
            compiler_params=pltpu.CompilerParams(vmem_limit_bytes=22 * 1024 * 1024),
            name="store",
        )(new_params, new_momentum, blocks)

    in_specs = (
        P(("rep", "fsdp"), None),
        P(),
        P(None, "fsdp", None),
        P(None, "fsdp", None),
        P("rep", None, "fsdp", None),
    )
    out_specs = (P(None, "fsdp", None), P(None, "fsdp", None), P(("rep", "fsdp"), None))
    return jax.shard_map(body, mesh=mesh, in_specs=in_specs, out_specs=out_specs, check_vma=False)
```
